32 devices in a mesh: pipe: 2 (over x), win: 4 (over y, core), fsdp: 4 (over z).
Axes of the slice: x: 2, y: 2, z: 4, core: 2. Of those that a mesh axis runs over, the one named last changes fastest.
Arguments:
- block_input: bfloat16 [64, 4, 49, 512], P('fsdp', 'win'), may hold values from -6 to 6
- out_grad: bfloat16 [64, 4, 49, 512], P('fsdp', 'win'), may hold values from -6 to 6
- norm_gains: bfloat16 [2, 2, 512], P('pipe', None, ('win', 'fsdp')), may hold values from 0.5 to 1.5
- norm_offsets: bfloat16 [2, 2, 512], P('pipe', None, ('win', 'fsdp')), may hold values from -2 to 2
- attend_weight: bfloat16 [2, 512, 1536], P('pipe', ('win', 'fsdp')), may hold values from -0.25 to 0.25
- row_biases: bfloat16 [2, 4, 512], P('pipe', None, ('win', 'fsdp')), may hold values from -2 to 2
- position_table: float32 [2, 169, 16], P('pipe'), may hold values from -2 to 302
- merge_weight: bfloat16 [2, 512, 512], P('pipe', ('win', 'fsdp')), may hold values from -0.5 to 0.5
- expand_weight: bfloat16 [2, 512, 2048], P('pipe', ('win', 'fsdp')), may hold values from -0.25 to 0.25
- hidden_biases: bfloat16 [2, 2048], P('pipe', ('win', 'fsdp')), may hold values from -2 to 2
- reduce_weight: bfloat16 [2, 2048, 512], P('pipe', ('win', 'fsdp')), may hold values from -0.125 to 0.125
- window_mask: int32 [4, 49, 49], P('win'), may hold values 0 or 1
- position_index: int32 [49, 49], replicated, may hold values from 0 to 168
Outputs:
- block_outputs: bfloat16 [2, 64, 4, 49, 512], P('pipe', 'fsdp', 'win')
- block_grads: float32 [2, 64, 4, 49, 512], P('pipe', 'fsdp', 'win')
- gain_grads: float32 [2, 2, 512], P('pipe', None, ('win', 'fsdp'))
- offset_grads: float32 [2, 2, 512], P('pipe', None, ('win', 'fsdp'))
- attend_grads: float32 [2, 512, 1536], P('pipe', ('win', 'fsdp'))
- bias_grads: float32 [2, 4, 512], P('pipe', None, ('win', 'fsdp'))
- table_grads: float32 [2, 169, 16], P('pipe')
- merge_grads: float32 [2, 512, 512], P('pipe', ('win', 'fsdp'))
- expand_grads: float32 [2, 512, 2048], P('pipe', ('win', 'fsdp'))
- hidden_grads: float32 [2, 2048], P('pipe', ('win', 'fsdp'))
- reduce_grads: float32 [2, 2048, 512], P('pipe', ('win', 'fsdp'))
The draws below stay inside these ranges and needn't reach their ends.
All inputs are finite; a program needn't handle non-finite values. No bound on the sum of `window_mask` on one device may be relied on, other than what follows from the above.
Results may differ from the reference program's by a relative error of at most 0.022.
Values may be sent and summed in bfloat16 or wider, within the bound.
A program may use at most 256 MiB of HBM per device.

```python
import math
import jax
import jax.numpy as jnp
from jax import lax

D = 512
HEADS = 16
FF = 2048
HEAD_DIM = 32
WIN = 49
TABLE = 169
WINDOWS = 4
SECTIONS = 2
IMAGES = 64


def draw_position_table(key, part):
    base_key = jax.random.fold_in(key, 11)
    jitter_key = jax.random.fold_in(base_key, 0)
    jitter = jax.random.uniform(jitter_key, (SECTIONS, TABLE, HEADS), jnp.float32, -2.0, 2.0)
    return jitter


def with_ends(drawn, own_key, smallest, largest):
    shape = drawn.shape
    index_at = [jax.random.randint(jax.random.fold_in(own_key, axis), (), 0, shape[axis]) for axis in range(len(shape))]
    drawn = drawn.at[tuple(index_at)].set(smallest)
    longest = shape.index(max(shape))
    index_at[longest] = (index_at[longest] + 1) % shape[longest]
    return drawn.at[tuple(index_at)].set(largest)


def spiked(array, key, source, target, shards_of, factor):
    def block_of(axis_at):
        return (jnp.arange(array.shape[axis_at]) // (array.shape[axis_at] // shards_of)).reshape((-1,) + (1,) * (array.ndim - 1 - axis_at))

    near = jax.random.permutation(key, shards_of)[block_of(target)]
    second = (block_of(target) + shards_of // 2) % shards_of
    return jnp.where((block_of(source) == near) | (block_of(source) == second), factor * array, array)


def steps_of(stream_key, extent, cuts, least, top_value):
    def one(axis_at, blocks):
        steps = jax.random.uniform(jax.random.fold_in(jax.random.fold_in(stream_key, 6), axis_at), (blocks,), jnp.float32, least / len(cuts), top_value / len(cuts))
        return jnp.repeat(jnp.exp(steps), extent[axis_at] // blocks).reshape((-1,) + (1,) * (len(extent) - axis_at - 1))

    gain = one(*cuts[0])
    for cut in cuts[1:]:
        gain = gain * one(*cut)
    return gain


def bell_draw(rng, extent, spread, most, cuts=(), kind=jnp.bfloat16):
    entries = spread * jax.random.normal(rng, extent, jnp.float32)
    if cuts:
        entries = entries * steps_of(rng, extent, cuts, -0.22, 0.18)
    return jnp.clip(entries, -most, most).astype(kind)


def noise_with(stream_key, extent, width, bound, shards, heavy, held_as=jnp.bfloat16):
    drawn = width * jax.random.normal(stream_key, extent, jnp.float32)
    if shards:
        drawn = drawn * steps_of(stream_key, extent, shards, -0.22, 0.18)
    return jnp.clip(spiked(drawn, jax.random.fold_in(stream_key, 3), *heavy), -bound, bound).astype(held_as)


def setup_inputs(seed: int = 0) -> dict:
    key_of = jax.random.split(jax.random.key(seed), 14)
    block_input = bell_draw(key_of[0], (IMAGES, WINDOWS, WIN, D), 1.0, 6.0, ((0, 4), (1, 4)))
    out_grad = noise_with(key_of[1], (IMAGES, WINDOWS, WIN, D), 1.0, 6.0, ((0, 4), (1, 4)), (0, 3, 4, 2.0))
    norm_gains = jnp.clip(1.0 + 0.1 * jax.random.normal(key_of[2], (SECTIONS, 2, D), jnp.float32), 0.5, 1.5).astype(jnp.bfloat16)
    norm_offsets = bell_draw(key_of[3], (SECTIONS, 2, D), 0.3, 2.0, ((0, 2), (2, 16)))
    attend_weight = bell_draw(key_of[4], (SECTIONS, D, 3 * D), D ** -0.5, 0.25, ((0, 2), (1, 16)))
    row_biases = bell_draw(key_of[5], (SECTIONS, 4, D), 0.3, 2.0, ((0, 2), (2, 16)))
    position_table = draw_position_table(jax.random.fold_in(key_of[13], 71), 0)
    merge_weight = bell_draw(key_of[7], (SECTIONS, D, D), (D // 4) ** -0.5, 0.5, ((0, 2), (1, 16)))
    expand_weight = bell_draw(key_of[8], (SECTIONS, D, FF), D ** -0.5, 0.25, ((0, 2), (1, 16)))
    hidden_biases = bell_draw(key_of[9], (SECTIONS, FF), 0.3, 2.0, ((0, 2), (1, 16)))
    reduce_weight = bell_draw(key_of[10], (SECTIONS, FF, D), FF ** -0.5, 0.125, ((0, 2), (1, 16)))
    window_mask = with_ends((jax.random.randint(key_of[11], (WINDOWS, WIN, WIN), 0, 4) < 1).astype(jnp.int32), jax.random.fold_in(key_of[11], 1), 0, 1)
    position_index = with_ends(jax.random.randint(key_of[12], (WIN, WIN), 0, TABLE), jax.random.fold_in(key_of[12], 1), 0, TABLE - 1).astype(jnp.int32)
    return {"block_input": block_input, "out_grad": out_grad, "norm_gains": norm_gains, "norm_offsets": norm_offsets, "attend_weight": attend_weight, "row_biases": row_biases, "position_table": position_table, "merge_weight": merge_weight, "expand_weight": expand_weight, "hidden_biases": hidden_biases, "reduce_weight": reduce_weight, "window_mask": window_mask, "position_index": position_index}


norm_eps = 1e-05
mask_level = -100.0

def widen(values):
    return lax.optimization_barrier(values).astype(jnp.float32)

def matmul(operand, other):
    return jnp.dot(operand, other, preferred_element_type=jnp.float32)

def contract_rows(operand, other):
    return lax.dot_general(operand, other, (((0,), (0,)), ((), ())), preferred_element_type=jnp.float32)

def contract_cols(operand, other):
    return lax.dot_general(operand, other, (((1,), (1,)), ((), ())), preferred_element_type=jnp.float32)

def layer_norm(values, norm_gain, norm_offset):
    average = lax.optimization_barrier(jnp.mean(values, axis=-1, keepdims=True))
    centered = values - average
    variance = lax.optimization_barrier(jnp.mean(centered * centered, axis=-1, keepdims=True))
    inv_std = lax.rsqrt(variance + norm_eps)
    unit_rows = centered * inv_std
    return (unit_rows * norm_gain + norm_offset, unit_rows, inv_std)

def norm_back(d_normed, unit_rows, inv_std, norm_gain):
    d_unit = d_normed * norm_gain
    term_one = lax.optimization_barrier(jnp.mean(d_unit, axis=-1, keepdims=True))
    term_two = lax.optimization_barrier(jnp.mean(d_unit * unit_rows, axis=-1, keepdims=True))
    return inv_std * (d_unit - term_one - unit_rows * term_two)

def gaussian_gate(before):
    cumulative = 0.5 * (1.0 + jax.scipy.special.erf(before * (1.0 / math.sqrt(2.0))))
    density = jnp.exp(-0.5 * before * before) * (1.0 / math.sqrt(2.0 * math.pi))
    return (before * cumulative, cumulative + before * density)

def image_roll(windows, amount):
    images = windows.shape[0]
    features = windows.shape[-1]
    window_grid = windows.reshape(images, 2, 2, 7, 7, features).transpose(0, 1, 3, 2, 4, 5).reshape(images, 14, 14, features)
    window_grid = jnp.roll(window_grid, (amount, amount), axis=(1, 2))
    return window_grid.reshape(images, 2, 7, 2, 7, features).transpose(0, 1, 3, 2, 4, 5).reshape(windows.shape)

def unchanged(values):
    return values

def roll_ahead(values):
    return image_roll(values, -3)

def roll_behind(values):
    return image_roll(values, 3)

def attention_forward(rolled, attend_w, row_bias, bias_heads, mask_term):
    grid_shape = rolled.shape
    score_scale = HEAD_DIM ** (-0.5)
    projected = matmul(rolled.reshape(-1, D), attend_w)
    split_shape = grid_shape[:3] + (HEADS, HEAD_DIM)
    query_rows = ((projected[:, :D] + row_bias[0]) * score_scale).astype(jnp.bfloat16).reshape(split_shape)
    key_rows = projected[:, D:2 * D].astype(jnp.bfloat16).reshape(split_shape)
    value_rows = (projected[:, 2 * D:] + row_bias[1]).astype(jnp.bfloat16).reshape(split_shape)
    scores = jnp.einsum('bwihd,bwjhd->bwhij', widen(query_rows), widen(key_rows)) + bias_heads + mask_term[None, :, None]
    row_max = lax.optimization_barrier(jnp.max(scores, axis=-1, keepdims=True))
    log_total = row_max + jnp.log(lax.optimization_barrier(jnp.sum(jnp.exp(scores - row_max), axis=-1, keepdims=True)))
    weights = jnp.exp(scores - log_total).astype(jnp.bfloat16)
    attended = jnp.einsum('bwhij,bwjhd->bwihd', widen(weights), widen(value_rows))
    return (attended.reshape(grid_shape).astype(jnp.bfloat16), query_rows, key_rows, value_rows, log_total)

def attention_backward(d_attended, query_rows, key_rows, value_rows, log_total, bias_heads, mask_term):
    score_scale = HEAD_DIM ** (-0.5)
    query_wide = widen(query_rows)
    key_wide = widen(key_rows)
    scores = jnp.einsum('bwihd,bwjhd->bwhij', query_wide, key_wide) + bias_heads + mask_term[None, :, None]
    probs = jnp.exp(scores - log_total)
    d_att = widen(d_attended.reshape(query_rows.shape))
    d_value = jnp.einsum('bwhij,bwihd->bwjhd', widen(probs.astype(jnp.bfloat16)), d_att)
    d_probs = jnp.einsum('bwihd,bwjhd->bwhij', d_att, widen(value_rows))
    d_scores = probs * (d_probs - lax.optimization_barrier(jnp.sum(probs * d_probs, axis=-1, keepdims=True)))
    d_bias = lax.optimization_barrier(jnp.sum(d_scores, axis=(0, 1)))
    scores_half = widen(d_scores.astype(jnp.bfloat16))
    d_query = jnp.einsum('bwhij,bwjhd->bwihd', scores_half, key_wide) * score_scale
    d_key = jnp.einsum('bwhij,bwihd->bwjhd', scores_half, query_wide)
    d_query = d_query.reshape(-1, D)
    d_key = d_key.reshape(-1, D)
    d_value = d_value.reshape(-1, D)
    d_proj = jnp.concatenate([d_query, d_key, d_value], axis=1).astype(jnp.bfloat16)
    return (d_proj, d_bias, lax.optimization_barrier(jnp.sum(d_query, axis=0)), lax.optimization_barrier(jnp.sum(d_value, axis=0)))

def block_forward(inputs, params, ahead, behind, bias_heads, mask_term):
    gains, offsets, attend_w, row_bias, merge_w, expand_w, hidden_bias, reduce_w = params
    grid_shape = inputs.shape
    inputs_flat = inputs.reshape(-1, D)
    normed_one = layer_norm(inputs_flat, gains[0], offsets[0])[0].astype(jnp.bfloat16)
    rolled = ahead(normed_one.reshape(grid_shape))
    attended, query_rows, key_rows, value_rows, log_total = attention_forward(rolled, attend_w, row_bias, bias_heads, mask_term)
    unrolled = behind(attended)
    middle = inputs_flat + matmul(unrolled.reshape(-1, D), merge_w) + row_bias[2]
    normed_two = layer_norm(middle, gains[1], offsets[1])[0].astype(jnp.bfloat16)
    before = matmul(normed_two, expand_w) + hidden_bias
    hidden = gaussian_gate(before)[0].astype(jnp.bfloat16)
    outputs = middle + matmul(hidden, reduce_w) + row_bias[3]
    retained = (inputs_flat, rolled, query_rows, key_rows, value_rows, log_total, unrolled, middle, normed_two, before)
    return (outputs.reshape(grid_shape), retained)

def block_backward(cotangent, retained, params, ahead, behind, bias_heads, mask_term):
    gains, offsets, attend_w, row_bias, merge_w, expand_w, hidden_bias, reduce_w = params
    inputs_flat, rolled, query_rows, key_rows, value_rows, log_total, unrolled, middle, normed_two, before = retained
    grid_shape = cotangent.shape
    cot_flat = cotangent.reshape(-1, D)
    active, gate_slope = gaussian_gate(before)
    hidden = active.astype(jnp.bfloat16)
    reduce_g = contract_rows(hidden, cot_flat)
    bias_three = lax.optimization_barrier(jnp.sum(widen(cot_flat), axis=0))
    d_before = (contract_cols(cot_flat, reduce_w) * gate_slope).astype(jnp.bfloat16)
    expand_g = contract_rows(normed_two, d_before)
    hidden_g = lax.optimization_barrier(jnp.sum(widen(d_before), axis=0))
    d_normed_two = contract_cols(d_before, expand_w)
    unit_two, inv_two = layer_norm(middle, gains[1], offsets[1])[1:]
    gain_two = lax.optimization_barrier(jnp.sum(d_normed_two * unit_two, axis=0))
    offset_two = lax.optimization_barrier(jnp.sum(d_normed_two, axis=0))
    d_middle = widen(cot_flat) + norm_back(d_normed_two, unit_two, inv_two, gains[1])
    d_branch = d_middle.astype(jnp.bfloat16)
    merge_g = contract_rows(unrolled.reshape(-1, D), d_branch)
    bias_two = lax.optimization_barrier(jnp.sum(d_middle, axis=0))
    d_unrolled = contract_cols(d_branch, merge_w).astype(jnp.bfloat16).reshape(grid_shape)
    d_attended = ahead(d_unrolled)
    d_proj, d_bias, query_g, value_g = attention_backward(d_attended, query_rows, key_rows, value_rows, log_total, bias_heads, mask_term)
    attend_g = contract_rows(rolled.reshape(-1, D), d_proj)
    d_rolled = contract_cols(d_proj, attend_w).astype(jnp.bfloat16).reshape(grid_shape)
    d_normed_one = widen(behind(d_rolled).reshape(-1, D))
    unit_one, inv_one = layer_norm(inputs_flat, gains[0], offsets[0])[1:]
    gain_one = lax.optimization_barrier(jnp.sum(d_normed_one * unit_one, axis=0))
    offset_one = lax.optimization_barrier(jnp.sum(d_normed_one, axis=0))
    d_inputs = d_middle + norm_back(d_normed_one, unit_one, inv_one, gains[0])
    gradients = (jnp.stack([gain_one, gain_two]), jnp.stack([offset_one, offset_two]), attend_g, jnp.stack([query_g, value_g, bias_two, bias_three]), d_bias, merge_g, expand_g, hidden_g, reduce_g)
    return (d_inputs.reshape(grid_shape), gradients)

def zero_grads():
    f32 = jnp.float32
    return (jnp.zeros((2, D), f32), jnp.zeros((2, D), f32), jnp.zeros((D, 3 * D), f32), jnp.zeros((4, D), f32), jnp.zeros((HEADS, WIN, WIN), f32), jnp.zeros((D, D), f32), jnp.zeros((D, FF), f32), jnp.zeros((FF,), f32), jnp.zeros((FF, D), f32))

def reference(block_input, out_grad, norm_gains, norm_offsets, attend_weight, row_biases, position_table, merge_weight, expand_weight, hidden_biases, reduce_weight, window_mask, position_index):
    f32 = jnp.float32

    def section_params(index):
        return (norm_gains[index].astype(f32), norm_offsets[index].astype(f32), attend_weight[index], row_biases[index].astype(f32), merge_weight[index], expand_weight[index], hidden_biases[index].astype(f32), reduce_weight[index])
    params_zero = section_params(0)
    params_one = section_params(1)
    bias_zero = position_table[0][position_index].transpose(2, 0, 1)
    bias_one = position_table[1][position_index].transpose(2, 0, 1)
    mask_one = mask_level * window_mask.astype(f32)
    mask_zero = jnp.zeros((WINDOWS, WIN, WIN), f32)
    block_size = math.gcd(IMAGES, 16)
    block_count = IMAGES // block_size
    inputs_all = block_input.reshape(block_count, block_size, WINDOWS, WIN, D)
    grads_all = out_grad.reshape(block_count, block_size, WINDOWS, WIN, D)

    def one_block(running, pair):
        input_part, grad_part = pair
        first_out, first_kept = block_forward(widen(input_part), params_zero, unchanged, unchanged, bias_zero, mask_zero)
        middle_half = first_out.astype(jnp.bfloat16)
        second_out, second_kept = block_forward(widen(middle_half), params_one, roll_ahead, roll_behind, bias_one, mask_one)
        final_half = second_out.astype(jnp.bfloat16)
        d_middle, grads_one = block_backward(grad_part, second_kept, params_one, roll_ahead, roll_behind, bias_one, mask_one)
        d_input, grads_zero = block_backward(d_middle.astype(jnp.bfloat16), first_kept, params_zero, unchanged, unchanged, bias_zero, mask_zero)
        running = (jax.tree.map(lambda earlier, update: earlier + update, running[0], grads_zero), jax.tree.map(lambda earlier, update: earlier + update, running[1], grads_one))
        return (running, (middle_half, final_half, d_input, d_middle))
    totals, stacked = lax.scan(one_block, (zero_grads(), zero_grads()), (inputs_all, grads_all))
    middles, finals, d_inputs, d_middles = stacked
    full_shape = (IMAGES, WINDOWS, WIN, D)
    block_outputs = jnp.stack([middles.reshape(full_shape), finals.reshape(full_shape)])
    block_grads = jnp.stack([d_inputs.reshape(full_shape), d_middles.reshape(full_shape)])

    def table_of(d_bias):
        flat_bias = d_bias.transpose(1, 2, 0).reshape(-1, HEADS)
        return jnp.zeros((TABLE, HEADS), f32).at[position_index.reshape(-1).astype(jnp.int32)].add(flat_bias)
    grads_zero, grads_one = totals

    def paired(index):
        return jnp.stack([grads_zero[index], grads_one[index]])
    table_grads = jnp.stack([table_of(grads_zero[4]), table_of(grads_one[4])])
    return (block_outputs, block_grads, paired(0), paired(1), paired(2), paired(3), table_grads, paired(5), paired(6), paired(7), paired(8))
```

```python
import math

import numpy as np
import jax
import jax.numpy as jnp
from jax import lax
from jax.experimental import pallas as pl
from jax.experimental.pallas import tpu as pltpu
from jax.sharding import PartitionSpec as P

f32 = jnp.float32
bf16 = jnp.bfloat16
D = 512
HEADS = 16
FF = 2048
TOK = 49
SLOT = 64
WINS = 8
RI = 208
R = 416
EPS = 1e-5
SCALE = 32 ** -0.5


def mm(a, b):
    return jnp.dot(a, b, preferred_element_type=f32)


def mm_t(a, b):
    return lax.dot_general(a, b, (((1,), (1,)), ((), ())), preferred_element_type=f32)


def t_mm(a, b):
    return lax.dot_general(a, b, (((0,), (0,)), ((), ())), preferred_element_type=f32)


def permutations():
    out = np.zeros((2, 4 * SLOT, RI), np.float32)
    for w in range(4):
        for t in range(TOK):
            out[0, w * SLOT + t, w * TOK + t] = 1.0
            i = ((w // 2) * 7 + t // 7 + 3) % 14
            j = ((w % 2) * 7 + t % 7 + 3) % 14
            ws, ts = (i // 7) * 2 + j // 7, (i % 7) * 7 + j % 7
            out[1, w * SLOT + t, ws * TOK + ts] = 1.0
    return out


def head_mask():
    return lax.broadcasted_iota(jnp.int32, (SLOT, 128), 1) // 32


def spread(block):
    lane = head_mask()
    zero = jnp.zeros_like(block)
    return jnp.concatenate([jnp.where(lane == h, block, zero) for h in range(4)], axis=0)


def gather_heads(full):
    lane = head_mask()
    out = jnp.zeros((SLOT, 128), f32)
    for h in range(4):
        out = jnp.where(lane == h, full[SLOT * h:SLOT * (h + 1)], out)
    return out


def build_bias(k):
    tabs, idx_ref, bn, bias = k.tabs, k.idx, k.bn, k.bias
    parts = []
    for s in range(2):
        tab = tabs[s]
        hi = tab.astype(bf16)
        rest = tab - hi.astype(f32)
        mid = rest.astype(bf16)
        low = (rest - mid.astype(f32)).astype(bf16)
        parts += [hi, mid, low]
    lhs = jnp.concatenate(parts, axis=0)
    rows_t = lax.broadcasted_iota(jnp.int32, (256, 128), 0)

    def one(i, carry):
        pick = (rows_t == idx_ref[pl.ds(i, 1), :]).astype(f32).astype(bf16)
        got = mm(lhs, pick)
        for s in range(2):
            p = got[48 * s:48 * (s + 1)]
            bn[s, pl.ds(i, 16, stride=SLOT), :] = p[:16] + p[16:32] + p[32:48]
        return carry

    for s in range(2):
        for h in range(HEADS):
            bn[s, SLOT * h + 48:SLOT * (h + 1), :] = jnp.zeros((16, 128), f32)
    lax.fori_loop(0, TOK, one, 0)
    dead = lax.broadcasted_iota(jnp.int32, (SLOT, 256), 0) >= TOK
    for s in range(2):
        for g in range(4):
            turned = jnp.transpose(bn[s, 256 * g:256 * (g + 1), :])[:SLOT]
            bias[s, :, 256 * g:256 * (g + 1)] = jnp.where(dead, -1e30, turned)


def row_loop(step, body):
    def one(i, carry):
        body(pl.ds(pl.multiple_of(i * step, step), step))
        return carry
    lax.fori_loop(0, R // step, one, 0)


def norm_rows(v, gain, offset):
    mean = jnp.mean(v, axis=-1, keepdims=True)
    cen = v - mean
    var = jnp.mean(cen * cen, axis=-1, keepdims=True)
    inv = lax.rsqrt(var + EPS)
    unit = cen * inv
    return unit * gain + offset, unit, inv


def attend_front(k, s):
    sm = k.small

    def ln(rows):
        y, unit, inv = norm_rows(k.u[rows], sm[s, 0:1, :], sm[s, 2:3, :])
        k.tmp[rows] = y.astype(bf16)
        k.n1[s, rows] = unit
        k.inv1[s, rows] = jnp.broadcast_to(inv, (32, 128))
    row_loop(32, ln)
    for m in range(2):
        k.rolled[s, 256 * m:256 * (m + 1), :] = mm(
            k.perm[s], k.tmp[RI * m:RI * (m + 1), :]).astype(bf16)


def project(k, s):
    def one(n, carry):
        cols = pl.ds(pl.multiple_of(n * 256, 256), 256)
        p = mm(k.rolled[s], k.wa[s, :, cols])
        half = pl.ds(pl.multiple_of((n % 2) * 256, 256), 256)
        add_q = jnp.where(n < 2, k.small[s, 4:5, half], 0.0)
        add_v = jnp.where(n >= 4, k.small[s, 5:6, half], 0.0)
        factor = jnp.where(n < 2, SCALE, 1.0)
        k.qkv[s, :, cols] = ((p + (add_q + add_v)) * factor).astype(bf16)
        return carry
    lax.fori_loop(0, 6, one, 0)


def attention(k, s):
    def one(w, carry):
        rows = pl.ds(pl.multiple_of(w * SLOT, SLOT), SLOT)
        for g in range(4):
            lanes = slice(128 * g, 128 * (g + 1))
            q = k.qkv[s, rows, 128 * g:128 * (g + 1)]
            key = k.qkv[s, rows, D + 128 * g:D + 128 * (g + 1)]
            val = k.qkv[s, rows, 2 * D + 128 * g:2 * D + 128 * (g + 1)]
            st = mm_t(key, spread(q)) + k.bias[s, :, 256 * g:256 * (g + 1)]
            if s == 1:
                mk = k.mask[w % 4]
                st = st + jnp.concatenate([mk, mk], axis=1)
            top = jnp.max(st, axis=0, keepdims=True)
            e = jnp.exp(st - top)
            p = e * (1.0 / jnp.sum(e, axis=0, keepdims=True))
            k.probs[s, w, :, 256 * g:256 * (g + 1)] = p
            k.att[rows, lanes] = gather_heads(t_mm(p.astype(bf16), val)).astype(bf16)
        return carry
    lax.fori_loop(0, WINS, one, 0)


def merge_rows(k, s):
    for m in range(2):
        k.unr[s, RI * m:RI * (m + 1), :] = t_mm(
            k.perm[s], k.att[256 * m:256 * (m + 1), :]).astype(bf16)
    sm = k.small

    def one(i, carry):
        rows = pl.ds(pl.multiple_of(i * RI, RI), RI)
        k.mid[rows] = mm(k.unr[s, rows, :], k.wa[s, :, 1536:2048])
        return carry
    lax.fori_loop(0, 2, one, 0)

    def ln(rows):
        middle = k.u[rows] + k.mid[rows] + sm[s, 6:7, :]
        y, unit, inv = norm_rows(middle, sm[s, 1:2, :], sm[s, 3:4, :])
        k.nrm2[s, rows] = y.astype(bf16)
        k.n2[s, rows] = unit
        k.inv2[s, rows] = jnp.broadcast_to(inv, (32, 128))
        k.acc[rows] = middle + sm[s, 7:8, :]
    row_loop(32, ln)


def expand(k, s):
    def one(n, carry):
        cols = pl.ds(pl.multiple_of(n * 256, 256), 256)
        wide = pl.ds(pl.multiple_of(2048 + n * 256, 256), 256)
        pre = mm(k.nrm2[s], k.wa[s, :, wide])
        hb = k.hbias[s, :, cols]
        x = pre + hb
        cdf = 0.5 * (1.0 + lax.erf(x * (1.0 / math.sqrt(2.0))))
        pdf = jnp.exp(-0.5 * x * x) * (1.0 / math.sqrt(2.0 * math.pi))
        k.hid[s, :, cols] = (x * cdf).astype(bf16)
        k.slope[s, :, cols] = (cdf + x * pdf).astype(k.slope.dtype)
        return carry
    lax.fori_loop(0, FF // 256, one, 0)


def reduce_rows(k, s):
    def one(n, carry):
        cols = pl.ds(pl.multiple_of(n * 256, 256), 256)
        k.acc[:, cols] = k.acc[:, cols] + mm(k.hid[s], k.wr[s, :, cols])
        return carry
    lax.fori_loop(0, 2, one, 0)
    for m in range(2):
        half = k.acc[RI * m:RI * (m + 1), :].astype(bf16)
        k.u[RI * m:RI * (m + 1), :] = half.astype(f32)
        k.send_out(s, m, mm(k.perm[0], half).astype(bf16))


def back_ff(k, s):
    def one(n, carry):
        cols = pl.ds(pl.multiple_of(n * 256, 256), 256)
        d = mm_t(k.cot[...], k.wr[s, cols, :]) * k.slope[s, :, cols].astype(f32)
        db = d.astype(bf16)
        k.wr[s, cols, :] = t_mm(k.hid[s, :, cols], k.cot[...]).astype(bf16)
        k.hid[s, :, cols] = db
        k.hgrad[:, cols] = jnp.sum(db.astype(f32), axis=0, keepdims=True)
        return carry
    lax.fori_loop(0, FF // 256, one, 0)
    for q in range(4):
        k.pk[s, 8 + q:9 + q, :] = k.hgrad[:, D * q:D * (q + 1)]
    k.ready(s, "red")

    def three(n, carry):
        rows = pl.ds(pl.multiple_of(n * 256, 256), 256)
        k.dn[:, rows] = mm_t(k.hid[s], k.wa[s, rows, 2048:4096])
        return carry
    lax.fori_loop(0, 2, three, 0)

    def two(n, carry):
        rows = pl.ds(pl.multiple_of(n * 128, 128), 128)
        k.wa[s, rows, 2048:4096] = t_mm(k.nrm2[s, :, rows], k.hid[s]).astype(bf16)
        return carry
    lax.fori_loop(0, 4, two, 0)
    k.ready(s, "exp")


def norm_back_rows(d, unit, inv, gain):
    dg = d * gain
    one = jnp.mean(dg, axis=-1, keepdims=True)
    two = jnp.mean(dg * unit, axis=-1, keepdims=True)
    return inv * (dg - one - unit * two)


def fold8(v):
    return (v[0:8] + v[8:16]) + (v[16:24] + v[24:32])


def back_mid(k, s):
    sm = k.small
    k.sums[...] = jnp.zeros_like(k.sums)

    def nb(rows):
        d = k.dn[rows]
        unit = k.n2[s, rows]
        c = k.cot[rows].astype(f32)
        dm = c + norm_back_rows(d, unit, k.inv2[s, rows, 0:1], sm[s, 1:2, :])
        k.dmid[rows] = dm
        k.tmp[rows] = dm.astype(bf16)
        k.sums[0] += fold8(d * unit)
        k.sums[1] += fold8(d)
        k.sums[2] += fold8(dm)
        k.sums[3] += fold8(c)
    row_loop(32, nb)
    for q, row in ((0, 1), (1, 3), (2, 6), (3, 7)):
        k.pk[s, row:row + 1, :] = jnp.sum(k.sums[q], axis=0, keepdims=True)

    for m in range(2):
        du = mm_t(k.tmp[RI * m:RI * (m + 1), :], k.wa[s, :, 1536:2048]).astype(bf16)
        k.att[256 * m:256 * (m + 1), :] = mm(k.perm[s], du).astype(bf16)

    def one(n, carry):
        rows = pl.ds(pl.multiple_of(n * 256, 256), 256)
        k.wa[s, rows, 1536:2048] = t_mm(k.unr[s, :, rows], k.tmp[...]).astype(bf16)
        return carry
    lax.fori_loop(0, 2, one, 0)
    k.ready(s, "mrg")


def back_attention(k, s):
    k.dbias[...] = jnp.zeros((SLOT, 1024), f32)
    k.qvsum[...] = jnp.zeros_like(k.qvsum)

    def one(w, carry):
        rows = pl.ds(pl.multiple_of(w * SLOT, SLOT), SLOT)
        for g in range(4):
            lanes = slice(128 * g, 128 * (g + 1))
            wide = slice(256 * g, 256 * (g + 1))
            q = k.qkv[s, rows, 128 * g:128 * (g + 1)]
            key = k.qkv[s, rows, D + 128 * g:D + 128 * (g + 1)]
            val = k.qkv[s, rows, 2 * D + 128 * g:2 * D + 128 * (g + 1)]
            da = spread(k.att[rows, lanes])
            p = k.probs[s, w, :, wide]
            dp = mm_t(val, da)
            ds = p * (dp - jnp.sum(p * dp, axis=0, keepdims=True))
            k.dbias[:, wide] += ds
            dsb = ds.astype(bf16)
            dv = mm(p.astype(bf16), da)
            dk = mm(dsb, spread(q))
            dq = gather_heads(t_mm(dsb, key)) * SCALE
            k.qkv[s, rows, 128 * g:128 * (g + 1)] = dq.astype(bf16)
            k.qkv[s, rows, D + 128 * g:D + 128 * (g + 1)] = dk.astype(bf16)
            k.qkv[s, rows, 2 * D + 128 * g:2 * D + 128 * (g + 1)] = dv.astype(bf16)
            k.qvsum[0, :, lanes] += fold8(dq[:32]) + fold8(dq[32:])
            k.qvsum[1, :, lanes] += fold8(dv[:32]) + fold8(dv[32:])
        return carry
    lax.fori_loop(0, WINS, one, 0)
    for q in range(2):
        k.pk[s, 4 + q:5 + q, :] = jnp.sum(k.qvsum[q], axis=0, keepdims=True)


def back_att_grads(k, s):
    def one(n, carry):
        rows = pl.ds(pl.multiple_of(n * 128, 128), 128)
        k.ga[s, rows, :] = t_mm(k.rolled[s, :, rows], k.qkv[s]).astype(bf16)
        return carry
    lax.fori_loop(0, 4, one, 0)
    k.ready(s, "att")


def back_input(k, s):
    sm = k.small

    def one(n, carry):
        rows = pl.ds(pl.multiple_of(n * 256, 256), 256)
        k.att[:, rows] = mm_t(k.qkv[s], k.wa[s, rows, 0:1536]).astype(bf16)
        return carry
    lax.fori_loop(0, 2, one, 0)
    for m in range(2):
        k.dn[RI * m:RI * (m + 1), :] = t_mm(k.perm[s], k.att[256 * m:256 * (m + 1), :])
    k.sums[...] = jnp.zeros_like(k.sums)

    def nb(rows):
        d = k.dn[rows].astype(bf16).astype(f32)
        unit = k.n1[s, rows]
        di = k.dmid[rows] + norm_back_rows(d, unit, k.inv1[s, rows, 0:1], sm[s, 0:1, :])
        k.cot[rows] = di.astype(bf16)
        k.sums[0] += fold8(d * unit)
        k.sums[1] += fold8(d)
    row_loop(32, nb)
    for q, row in ((0, 0), (1, 2)):
        k.pk[s, row:row + 1, :] = jnp.sum(k.sums[q], axis=0, keepdims=True)
    for m in range(2):
        k.send_grad(s, m, mm(k.perm[0], k.cot[RI * m:RI * (m + 1), :]).astype(bf16))


def table_grad(k, s):
    bn = k.bn
    for g in range(4):
        bn[0, 256 * g:256 * (g + 1), 0:SLOT] = jnp.transpose(k.dbias[:, 256 * g:256 * (g + 1)])
    rows_t = lax.broadcasted_iota(jnp.int32, (256, 128), 0)
    lane = lax.broadcasted_iota(jnp.int32, (16, 128), 1)

    def one(i, acc):
        pick = (rows_t == k.idx[pl.ds(i, 1), :]).astype(f32).astype(bf16)
        x = jnp.where(lane < TOK, bn[0, pl.ds(i, 16, stride=SLOT), :], 0.0)
        hi = x.astype(bf16)
        low = (x - hi.astype(f32)).astype(bf16)
        got = mm_t(jnp.concatenate([hi, low], axis=0), pick)
        return acc + got[:16] + got[16:]
    total = lax.fori_loop(0, TOK, one, jnp.zeros((16, 256), f32))
    k.pk[s, 12:20, 0:256] = total[:8]
    k.pk[s, 12:20, 256:512] = total[8:]


def load_input(k, src, dst_f32=None, dst_b16=None):
    tok = lax.broadcasted_iota(jnp.int32, (256, D), 0) % SLOT
    for m in range(2):
        x = src[m].reshape(256, D)
        x = jnp.where(tok < TOK, x, jnp.zeros_like(x))
        c = t_mm(k.perm[0], x)
        if dst_f32 is not None:
            dst_f32[RI * m:RI * (m + 1), :] = c
        if dst_b16 is not None:
            dst_b16[RI * m:RI * (m + 1), :] = c.astype(bf16)


MESH = pl.DeviceIdType.MESH
PIECES = (
    ("s", 0, 128), ("a", 0, 512), ("a", 512, 1024), ("a", 1024, 1536), ("a", 1536, 2048),
    ("a", 2048, 3072), ("a", 3072, 4096), ("r", 0, 256), ("r", 256, 512),
)
SHARD = {"s": 16, "a": 32, "r": 128}
FINISHED = {
    "red": (("r", 0, 256), ("r", 256, 512)),
    "exp": (("a", 2048, 3072), ("a", 3072, 4096)),
    "mrg": (("a", 1536, 2048),),
    "att": (("a", 0, 512), ("a", 512, 1024), ("a", 1024, 1536)),
}
PER_BLOCK = 8


def scratch():
    V = pltpu.VMEM
    S = pltpu.SemaphoreType.DMA
    return dict(
        wa=V((2, 512, 4096), bf16), wr=V((2, 2048, 512), bf16), ws=V((2, 256, 128), bf16),
        ga=V((2, 512, 1536), bf16),
        xin=V((2, 4, SLOT, D), bf16), cin=V((2, 4, SLOT, D), bf16), mask=V((4, SLOT, 128), bf16),
        tabs=V((2, 16, 256), f32), small=V((2, 8, D), f32), hbias=V((2, 1, FF), f32),
        u=V((R, D), f32), tmp=V((R, D), bf16), acc=V((R, D), f32), dn=V((R, D), f32),
        n1=V((2, R, D), f32), inv1=V((2, R, 128), f32), n2=V((2, R, D), f32), inv2=V((2, R, 128), f32),
        rolled=V((2, 512, D), bf16), qkv=V((2, 512, 3 * D), bf16), probs=V((2, WINS, SLOT, 1024), f32),
        att=V((512, D), bf16), unr=V((2, R, D), bf16), nrm2=V((2, R, D), bf16),
        hid=V((2, R, FF), bf16), slope=V((2, R, FF), bf16), cot=V((R, D), bf16),
        sums=V((4, 8, D), f32), qvsum=V((2, 8, D), f32), hgrad=V((1, FF), f32),
        bias=V((2, SLOT, 1024), f32), bn=V((2, 1024, 128), f32), dbias=V((SLOT, 1024), f32),
        pk=V((2, 24, D), f32), pk_c=V((2, 24, D), f32), pk_y=V((2, 24, D), f32), pk_z=V((4, 24, D), f32),
        got_c=V((2, 24, D), f32), got_y=V((2, 24, D), f32), got_x=V((24, D), f32),
        ca=V((2, 256, 4096), bf16), cr=V((2, 1024, 512), bf16),
        ya=V((2, 64, 4096), bf16), yr=V((2, 256, 512), bf16),
        yba=V((64, 4096), bf16), ybr=V((256, 512), bf16),
        xba=V((2, 64, 4096), bf16), xbr=V((2, 256, 512), bf16),
        xaa=V((64, 4096), bf16), xar=V((256, 512), bf16),
        za=V((3, 32, 4096), bf16), zr=V((3, 128, 512), bf16),
        g_send=S((len(PIECES), 11)), g_recv=S((len(PIECES), 11)), g_own=S((len(PIECES),)),
        r_send=S((2 * PER_BLOCK, 10)), r_recv=S((2 * PER_BLOCK, 10)),
        p_send=S((2, 6)), p_recv=S((2, 6)),
        i_send=S((3, 3)), i_recv=S((3, 3)), i_own=S((3,)),
        t_send=S((1,)), t_recv=S((1,)), t_own=S((1,)),
        o_send=S((2, 2, 4)), o_recv=S((2, 8)),
    )


ALIASES = {"mid": "dn", "dmid": "u"}


class Kernel:
    def __init__(self, refs, sub):
        self.__dict__.update(refs)
        for name, other in ALIASES.items():
            setattr(self, name, getattr(self, other))
        self.px = lax.axis_index("pipe")
        self.w = lax.axis_index("win")
        self.z = lax.axis_index("fsdp")
        self.y, self.c = self.w // 2, self.w % 2
        self.g, self.low = self.z // sub, self.z % sub
        self.sub = sub
        self.wy = (1 - self.y) * 2 + self.c
        self.wc = self.y * 2 + 1 - self.c
        self.wyc = (1 - self.y) * 2 + 1 - self.c
        self.own, self.other = self.px, 1 - self.px
        self.at_x = self.device(1 - self.px, self.w, self.z)
        self.at_y = self.device(self.px, self.wy, self.z)
        self.at_c = self.device(self.px, self.wc, self.z)
        self.flying = []
        self.pending = []
        self.reduced = 0

    def device(self, pipe, win, fsdp):
        return {"pipe": pipe, "win": win, "fsdp": fsdp}

    def at_z(self, d):
        return self.device(self.px, self.w, ((self.g + d) % 4) * self.sub + self.low)

    def barrier(self):
        sem = pltpu.get_barrier_semaphore()
        peers = [self.at_z(d) for d in (1, 2, 3)]
        for dw in range(4):
            for dp in range(2):
                if dw or dp:
                    peers.append(self.device((self.px + dp) % 2, (self.w + dw) % 4, self.z))
        for peer in peers:
            pl.semaphore_signal(sem, inc=1, device_id=peer, device_id_type=MESH)
        pl.semaphore_wait(sem, len(peers))

    def move(self, src, dst, send, recv, device):
        return pltpu.make_async_remote_copy(
            src_ref=src, dst_ref=dst, send_sem=send, recv_sem=recv, device_id=device, device_id_type=MESH)

    def inputs(self, start):
        for which, (src, dst) in enumerate(((self.x_h, self.xin), (self.c_h, self.cin), (self.m_h, self.mask))):
            def part(v):
                return src if which == 2 else src.at[pl.ds(8 * self.px + 2 * v, 2)]

            def place(v):
                return dst.at[v] if which == 2 else dst.at[:, v]
            if start:
                pltpu.make_async_copy(part(self.w), place(self.w), self.i_own.at[which]).start()
                for d in (1, 2, 3):
                    v = (self.w + d) % 4
                    self.move(part(v), place(self.w), self.i_send.at[which, d - 1], self.i_recv.at[which, d - 1],
                              self.device(self.px, v, self.z)).start()

    def input_done(self, which):
        src, dst = ((self.x_h, self.xin), (self.c_h, self.cin), (self.m_h, self.mask))[which]
        mine = src if which == 2 else src.at[pl.ds(8 * self.px + 2 * self.w, 2)]

        def place(v):
            return dst.at[v] if which == 2 else dst.at[:, v]
        pltpu.make_async_copy(mine, place(self.w), self.i_own.at[which]).wait()
        for d in (1, 2, 3):
            copy = self.move(mine, place((self.w + 4 - d) % 4), self.i_send.at[which, d - 1],
                             self.i_recv.at[which, d - 1], self.at_x)
            copy.wait_recv()
            copy.wait_send()

    def tables(self, start):
        own = pltpu.make_async_copy(self.tab_h, self.tabs.at[self.px], self.t_own.at[0])
        if start:
            own.start()
            self.move(self.tab_h, self.tabs.at[self.px], self.t_send.at[0], self.t_recv.at[0], self.at_x).start()
        else:
            own.wait()
            copy = self.move(self.tab_h, self.tabs.at[self.other], self.t_send.at[0], self.t_recv.at[0], self.at_x)
            copy.wait_recv()
            copy.wait_send()

    def spot(self, e, block, row, rows):
        kind, lo, hi = PIECES[e]
        ref = {"s": self.ws, "a": self.wa, "r": self.wr}[kind]
        rows_at = pl.ds(pl.multiple_of(row, 16), rows)
        return ref.at[block, rows_at, pl.ds(lo, hi - lo)]

    def line(self, e, block, win, half=None):
        rows = SHARD[PIECES[e][0]] * 4
        if half is None:
            return self.spot(e, block, win * rows, rows)
        return self.spot(e, block, win * rows + half * (rows // 2), rows // 2)

    def shard_src(self, e):
        kind, lo, hi = PIECES[e]
        if kind == "s":
            return self.sp_h
        if kind == "r":
            return self.red_h.at[:, pl.ds(lo, hi - lo)]
        for ref, at in ((self.att_h, 0), (self.mrg_h, 1536), (self.exp_h, 2048)):
            if at <= lo < at + ref.shape[1]:
                return ref.at[:, pl.ds(lo - at, hi - lo)]

    def shard_spot(self, e, g):
        rows = SHARD[PIECES[e][0]]
        return self.spot(e, self.own, (self.w * 4 + g) * rows, rows)

    def send(self, e, n, src, device):
        self.move(src, src, self.g_send.at[e, n], self.g_recv.at[e, n], device).start()

    def landed(self, e, n, place):
        self.move(place, place, self.g_send.at[e, 0], self.g_recv.at[e, n], self.at_x).wait_recv()

    def gather_start(self, e):
        src = self.shard_src(e)
        pltpu.make_async_copy(src, self.shard_spot(e, self.g), self.g_own.at[e]).start()
        for d in (1, 2, 3):
            self.move(src, self.shard_spot(e, self.g), self.g_send.at[e, d - 1], self.g_recv.at[e, d - 1],
                      self.at_z(d)).start()

    def gather_one(self, e):
        pltpu.make_async_copy(self.shard_src(e), self.shard_spot(e, self.g), self.g_own.at[e]).wait()
        for d in (1, 2, 3):
            self.landed(e, d - 1, self.shard_spot(e, (self.g + 4 - d) % 4))
        mine = self.line(e, self.own, self.w)
        self.send(e, 3, mine, self.at_x)
        self.send(e, 4, mine, self.at_y)
        self.send(e, 5, mine, self.at_c)

    def gather_two(self, e):
        got = self.line(e, self.other, self.w)
        self.landed(e, 3, got)
        self.send(e, 6, self.line(e, self.other, self.w, 0), self.at_y)
        self.send(e, 7, got, self.at_c)
        got = self.line(e, self.own, self.wy)
        self.landed(e, 4, got)
        self.send(e, 8, self.line(e, self.own, self.wy, 1), self.at_x)
        self.send(e, 9, got, self.at_c)

    def gather_three(self, e):
        self.landed(e, 6, self.line(e, self.other, self.wy, 0))
        self.landed(e, 8, self.line(e, self.other, self.wy, 1))
        self.send(e, 10, self.line(e, self.other, self.wy), self.at_c)

    def gathered(self, e, block):
        mine = self.px == block
        self.landed(e, jnp.where(mine, 5, 7), self.line(e, block, self.wc))
        self.landed(e, jnp.where(mine, 9, 10), self.line(e, block, self.wyc))

    def tick(self, i):
        n = len(PIECES)
        if i < n:
            self.gather_one(i)
        if 0 <= i - 1 < n:
            self.gather_two(i - 1)
        if 0 <= i - 2 < n:
            self.gather_three(i - 2)

    def gather_sent(self, e):
        mine = self.line(e, self.own, self.w)
        half = self.line(e, self.own, self.w, 0)
        shard = self.shard_spot(e, self.g)
        for n in range(11):
            src = shard if n < 3 else half if n in (6, 8) else mine
            self.move(src, src, self.g_send.at[e, n], self.g_recv.at[e, n], self.at_x).wait_send()

    def decode(self):
        for s in range(2):
            for win in range(4):
                total = jnp.zeros((8, 128), f32)
                for g in range(4):
                    r = win * 4 + g
                    total = total + self.ws[s, 16 * r:16 * r + 16, :].astype(f32)[:8]
                    self.hbias[s, :, 128 * r:128 * (r + 1)] = self.ws[s, 16 * r:16 * r + 16, :].astype(f32)[8:9]
                self.small[s, :, 128 * win:128 * (win + 1)] = total

    def send_out(self, s, m, value):
        self.emit(0, s, m, value)

    def send_grad(self, s, m, value):
        self.emit(1, s, m, value)

    def emit(self, which, s, m, value):
        stage = (self.xin, self.cin)[s]
        dst = (self.out_h, self.grad_h)[which]
        if m == 0 and which == 1:
            self.emitted(0, s)
        for v in range(4):
            stage[m, v] = value[SLOT * v:SLOT * (v + 1)]
        if m == 0:
            return
        at = pl.ds(8 * self.px + 2 * self.w, 2)
        for v in range(4):
            here = (self.px == s) & (self.w == v)
            recv = self.o_recv.at[which, self.px * 4 + self.w]

            @pl.when(here)
            def _():
                pltpu.make_async_copy(stage.at[:, v], dst.at[at], recv).start()

            @pl.when(jnp.logical_not(here))
            def _():
                self.move(stage.at[:, v], dst.at[at], self.o_send.at[which, s, v], recv,
                          self.device(s, v, self.z)).start()

    def emitted(self, which, s):
        stage = (self.xin, self.cin)[s]
        dst = (self.out_h, self.grad_h)[which]
        at = pl.ds(8 * self.px + 2 * self.w, 2)
        for v in range(4):
            here = (self.px == s) & (self.w == v)
            recv = self.o_recv.at[which, self.px * 4 + self.w]

            @pl.when(here)
            def _():
                pltpu.make_async_copy(stage.at[:, v], dst.at[at], recv).wait()

            @pl.when(jnp.logical_not(here))
            def _():
                self.move(stage.at[:, v], dst.at[at], self.o_send.at[which, s, v], recv,
                          self.device(s, v, self.z)).wait_send()

    def arrived(self, which):
        dst = (self.out_h, self.grad_h)[which]
        for p in range(2):
            for v in range(4):
                from_here = (self.px == p) & (self.w == v)

                @pl.when(jnp.logical_not(from_here))
                def _():
                    place = dst.at[pl.ds(8 * p + 2 * v, 2)]
                    self.move(place, place, self.o_send.at[which, 0, 0], self.o_recv.at[which, p * 4 + v],
                              self.at_x).wait_recv()

    def ready(self, s, kind):
        fresh = []
        for piece in FINISHED[kind]:
            fresh.append([s, piece, self.reduced, 0])
            self.reduced += 1
        self.pump()
        for job in fresh:
            self.advance(job)
        self.flying += fresh

    def pump(self):
        for job in self.flying:
            self.advance(job)
        self.flying = [job for job in self.flying if job[3] < 5]

    def advance(self, job):
        (self.reduce_zero, self.reduce_one, self.reduce_two, self.reduce_three, self.reduce_four)[job[3]](*job[:3])
        job[3] += 1

    def part(self, piece):
        kind, lo, hi = piece
        grads = self.wr if kind == "r" else self.ga if hi <= 1536 else self.wa
        bufs = (self.cr, self.yr, self.ybr, self.xbr, self.xar, self.zr) if kind == "r" else (
            self.ca, self.ya, self.yba, self.xba, self.xaa, self.za)
        return grads, bufs, SHARD[kind], pl.ds(lo, hi - lo)

    def add(self, grads, s, row, src, rows, cols):
        step = 16 if cols.size > 512 else 32

        def one(i, carry):
            at = pl.ds(pl.multiple_of(row + i * step, 16), step)
            here = pl.ds(pl.multiple_of(i * step, 16), step)
            grads[s, at, cols] = (grads[s, at, cols].astype(f32) + src[here, cols].astype(f32)).astype(bf16)
            return carry
        lax.fori_loop(0, rows // step, one, 0)

    def cut(self, grads, s, row, rows, cols):
        return grads.at[s, pl.ds(pl.multiple_of(row, 16), rows), cols]

    def throw(self, q, n, src, dst, device):
        self.move(src, dst, self.r_send.at[q, n], self.r_recv.at[q, n], device).start()

    def caught(self, q, n, place):
        self.move(place, place, self.r_send.at[q, n], self.r_recv.at[q, n], self.at_x).wait_recv()

    def thrown(self, q, n, src):
        self.move(src, src, self.r_send.at[q, n], self.r_recv.at[q, n], self.at_x).wait_send()

    def reduce_zero(self, s, piece, q):
        grads, bufs, rps, cols = self.part(piece)
        lr = 4 * rps
        for v in range(2):
            src = self.cut(grads, s, (2 * v + 1 - self.c) * lr, lr, cols)
            self.throw(q, v, src, bufs[0].at[s, pl.ds(v * lr, lr), cols], self.at_c)

    def reduce_one(self, s, piece, q):
        grads, bufs, rps, cols = self.part(piece)
        lr, half = 4 * rps, 2 * rps
        for v in range(2):
            place = bufs[0].at[s, pl.ds(v * lr, lr), cols]
            self.caught(q, v, place)
            self.add(grads, s, (2 * v + self.c) * lr, bufs[0].at[s, pl.ds(v * lr, lr)], lr, cols)
        self.throw(q, 2, self.cut(grads, s, self.wy * lr, half, cols), bufs[1].at[s, :, cols], self.at_y)

        @pl.when(self.px != s)
        def _():
            self.throw(q, 3, self.cut(grads, s, self.w * lr + half, half, cols), bufs[3].at[0, :, cols], self.at_x)
            self.throw(q, 4, self.cut(grads, s, self.wy * lr + half, half, cols), bufs[3].at[1, :, cols], self.at_x)

    def reduce_two(self, s, piece, q):
        grads, bufs, rps, cols = self.part(piece)
        lr, half = 4 * rps, 2 * rps
        self.caught(q, 2, bufs[1].at[s, :, cols])
        self.add(grads, s, self.w * lr, bufs[1].at[s], half, cols)

        @pl.when(self.px != s)
        def _():
            self.throw(q, 5, self.cut(grads, s, self.w * lr, half, cols), bufs[4].at[:, cols], self.at_x)

        @pl.when(self.px == s)
        def _():
            for n, win in ((0, self.w), (1, self.wy)):
                self.caught(q, 3 + n, bufs[3].at[n, :, cols])
                self.add(grads, s, win * lr + half, bufs[3].at[n], half, cols)
            self.throw(q, 6, self.cut(grads, s, self.wy * lr + half, half, cols), bufs[2].at[:, cols], self.at_y)

    def reduce_three(self, s, piece, q):
        grads, bufs, rps, cols = self.part(piece)
        lr, half = 4 * rps, 2 * rps

        @pl.when(self.px == s)
        def _():
            self.caught(q, 5, bufs[4].at[:, cols])
            self.add(grads, s, self.w * lr, bufs[4], half, cols)
            self.caught(q, 6, bufs[2].at[:, cols])
            self.add(grads, s, self.w * lr + half, bufs[2], half, cols)
            for d in (1, 2, 3):
                row = (self.w * 4 + (self.g + d) % 4) * rps
                self.throw(q, 6 + d, self.cut(grads, s, row, rps, cols), bufs[5].at[d - 1, :, cols], self.at_z(d))

    def reduce_four(self, s, piece, q):
        grads, bufs, rps, cols = self.part(piece)
        lr, half = 4 * rps, 2 * rps
        kind, lo, hi = piece
        out, at = self.o_red, 0
        if kind == "a":
            out, at = ((self.o_att, 0), (self.o_mrg, 1536), (self.o_exp, 2048))[
                0 if lo < 1536 else 1 if lo < 2048 else 2]
        to = pl.ds(lo - at, hi - lo)

        @pl.when(self.px == s)
        def _():
            for d in (1, 2, 3):
                self.caught(q, 6 + d, bufs[5].at[d - 1, :, cols])
            base = (self.w * 4 + self.g) * rps

            def one(i, carry):
                rows = pl.ds(pl.multiple_of(i * 16, 16), 16)
                total = grads[s, pl.ds(pl.multiple_of(base + i * 16, 16), 16), cols].astype(f32)
                for n in range(3):
                    total = total + bufs[5][n, rows, cols].astype(f32)
                out[rows, to] = total
                return carry
            lax.fori_loop(0, rps // 16, one, 0)

        for n in (0, 1):
            self.thrown(q, n, self.cut(grads, s, 0, lr, cols))
        self.thrown(q, 2, self.cut(grads, s, 0, half, cols))

        @pl.when(self.px != s)
        def _():
            for n in (3, 4, 5):
                self.thrown(q, n, self.cut(grads, s, 0, half, cols))

        @pl.when(self.px == s)
        def _():
            self.thrown(q, 6, self.cut(grads, s, 0, half, cols))
            for n in (7, 8, 9):
                self.thrown(q, n, self.cut(grads, s, 0, rps, cols))

    def small_step(self, s, step):
        def copy(n, src, dst, device):
            return self.move(src, dst, self.p_send.at[s, n], self.p_recv.at[s, n], device)
        first = copy(0, self.pk.at[s], self.got_c.at[s], self.at_c)
        second = copy(1, self.pk_c.at[s], self.got_y.at[s], self.at_y)
        third = copy(2, self.pk_y.at[s], self.got_x, self.at_x)
        last = [copy(2 + d, self.pk_z.at[self.g], self.pk_z.at[self.g], self.at_z(d)) for d in (1, 2, 3)]
        if step == 0:
            first.start()
        if step == 1:
            first.wait_recv()
            self.pk_c[s] = self.pk[s] + self.got_c[s]
            second.start()
        if step == 2:
            second.wait_recv()
            self.pk_y[s] = self.pk_c[s] + self.got_y[s]

            @pl.when(self.px != s)
            def _():
                third.start()
        if step == 3:
            @pl.when(self.px == s)
            def _():
                third.wait_recv()
                self.pk_z[self.g] = self.pk_y[s] + self.got_x[...]
                for c in last:
                    c.start()
        if step == 4:
            first.wait_send()
            second.wait_send()

            @pl.when(self.px != s)
            def _():
                third.wait_send()

            @pl.when(self.px == s)
            def _():
                for d in (1, 2, 3):
                    place = self.pk_z.at[(self.g + 4 - d) % 4]
                    copy(2 + d, place, place, self.at_x).wait_recv()
                    last[d - 1].wait_send()
                self.o_pk[...] = ((self.pk_z[0] + self.pk_z[1]) + self.pk_z[2]) + self.pk_z[3]


def program(k):
    k.barrier()
    for e in range(4):
        k.gather_start(e)
        if e == 0:
            k.inputs(True)
            k.tables(True)
    for e in range(4, len(PIECES)):
        k.gather_start(e)
    k.tables(False)
    k.tick(0)
    build_bias(k)
    k.tick(1)
    k.tick(2)
    for which in range(3):
        k.input_done(which)
    for s in range(2):
        k.gathered(0, s)
    k.decode()
    load_input(k, k.xin, dst_f32=k.u)
    load_input(k, k.cin, dst_b16=k.cot)
    for s in range(2):
        attend_front(k, s)
        for e in (1, 2, 3):
            if s == 0:
                k.tick(e + 2)
        for e in (1, 2, 3):
            k.gathered(e, s)
        project(k, s)
        attention(k, s)
        if s == 0:
            k.tick(6)
        k.gathered(4, s)
        merge_rows(k, s)
        if s == 0:
            k.tick(7)
            k.tick(8)
        k.gathered(5, s)
        k.gathered(6, s)
        expand(k, s)
        if s == 0:
            k.tick(9)
            k.tick(10)
        k.gathered(7, s)
        k.gathered(8, s)
        reduce_rows(k, s)
    for e in range(len(PIECES)):
        k.gather_sent(e)
    for s in (1, 0):
        back_ff(k, s)
        back_mid(k, s)
        back_attention(k, s)
        back_att_grads(k, s)
        table_grad(k, s)
        back_input(k, s)
        k.small_step(s, 0)
        if s == 1:
            k.pump()
            for step in range(1, 5):
                k.small_step(s, step)
    step = 1
    while k.flying or step < 5:
        k.pump()
        if step < 5:
            k.small_step(0, step)
        step += 1
    k.arrived(0)
    k.arrived(1)
    k.emitted(1, 1)
    k.emitted(1, 0)


INPUTS = ("x_h", "c_h", "att_h", "mrg_h", "exp_h", "red_h", "sp_h", "tab_h", "m_h", "idx", "perm")
OUTPUTS = ("out_h", "grad_h", "o_att", "o_mrg", "o_exp", "o_red", "o_pk")


def both_blocks(sub, *operands):
    names = scratch()

    def body(*refs):
        all_names = INPUTS + OUTPUTS + tuple(names)
        program(Kernel(dict(zip(all_names, refs)), sub))
    S = jax.ShapeDtypeStruct
    images = operands[0].shape[0]
    anywhere = pl.BlockSpec(memory_space=pl.ANY)
    local = pl.BlockSpec(memory_space=pltpu.VMEM)
    return pl.pallas_call(
        body,
        out_shape=(
            S((images, SLOT, D), bf16), S((images, SLOT, D), bf16), S((32, 1536), f32), S((32, 512), f32),
            S((32, 2048), f32), S((128, 512), f32), S((24, D), f32)),
        in_specs=[anywhere] * 9 + [local] * 2,
        out_specs=[anywhere] * 2 + [local] * 5,
        scratch_shapes=[names[n] for n in names],
        compiler_params=pltpu.CompilerParams(
            collective_id=0, has_side_effects=True, vmem_limit_bytes=67043328),
    )(*operands)


def shards(block_input, out_grad, norm_gains, norm_offsets, attend_weight, row_biases, position_table,
           merge_weight, expand_weight, hidden_biases, reduce_weight, window_mask, position_index):
    fsdp = lax.axis_size("fsdp")
    sub = fsdp // 4
    z = lax.axis_index("fsdp")
    group = z // sub
    groups = [[g * sub + i for i in range(sub)] for g in range(4)]

    def whole(shard, axis):
        if sub == 1:
            return shard
        return lax.all_gather(shard, "fsdp", axis=axis, axis_index_groups=groups, tiled=True)

    att = whole(attend_weight[0], 0)
    mrg = whole(merge_weight[0], 0)
    exp = whole(expand_weight[0], 0)
    red = whole(reduce_weight[0], 0)
    rows = jnp.concatenate([norm_gains[0], norm_offsets[0], row_biases[0]], axis=0)
    rows = whole(rows, 1)
    hid = whole(hidden_biases[0], 0)
    at = jnp.arange(128, dtype=jnp.int32) // 32 == group
    placed = jnp.where(at[None, :], jnp.tile(rows, (1, 4)), jnp.zeros((), bf16))
    small = jnp.concatenate([placed, hid[None, :], jnp.zeros((7, 128), bf16)], axis=0)
    table = jnp.pad(position_table[0].T, ((0, 0), (0, 256 - position_table.shape[1])))
    mask = jnp.pad(jnp.where(window_mask[0].T > 0, -100.0, 0.0).astype(bf16), ((0, SLOT - TOK), (0, SLOT - TOK)))
    mask = jnp.concatenate([mask, mask], axis=1)
    idx = jnp.pad(position_index, ((0, 56 - TOK), (0, 128 - TOK)), constant_values=-1)
    perm = jnp.asarray(permutations(), bf16)
    spread_out = ((0, 0), (0, SLOT - TOK), (0, 0))
    x = jnp.pad(block_input[:, 0], spread_out)
    c = jnp.pad(out_grad[:, 0], spread_out)
    out, grad, g_att, g_mrg, g_exp, g_red, pk = both_blocks(
        sub, x, c, att, mrg, exp, red, small, table, mask, idx, perm)

    def mine(total, axis):
        if sub == 1:
            return total
        return lax.psum_scatter(total, "fsdp", scatter_dimension=axis, axis_index_groups=groups, tiled=True)

    def spread_sum(total):
        if sub == 1:
            return total
        return lax.psum(total, "fsdp", axis_index_groups=groups)

    pk = spread_sum(pk)
    r = lax.axis_index("win") * fsdp + z
    width = D // (4 * fsdp)
    sums = lax.dynamic_slice(pk, (0, r * width), (8, width))
    hidden = lax.dynamic_slice(pk[8:12].reshape(1, FF), (0, r * 4 * width), (1, 4 * width))
    tab = jnp.concatenate([pk[12:20, :256], pk[12:20, 256:]], axis=0)[:, :position_table.shape[1]].T
    return (
        out[:, :TOK].reshape((1,) + block_input.shape),
        grad[:, :TOK].astype(f32).reshape((1,) + block_input.shape),
        sums[None, 0:2], sums[None, 2:4], mine(g_att, 0)[None], sums[None, 4:8], tab[None],
        mine(g_mrg, 0)[None], mine(g_exp, 0)[None], hidden, mine(g_red, 0)[None],
    )


def solution(mesh):
    placed = (
        P("fsdp", "win", None, None),
        P("fsdp", "win", None, None),
        P("pipe", None, ("win", "fsdp")),
        P("pipe", None, ("win", "fsdp")),
        P("pipe", ("win", "fsdp"), None),
        P("pipe", None, ("win", "fsdp")),
        P("pipe", None, None),
        P("pipe", ("win", "fsdp"), None),
        P("pipe", ("win", "fsdp"), None),
        P("pipe", ("win", "fsdp")),
        P("pipe", ("win", "fsdp"), None),
        P("win", None, None),
        P(),
    )
    return jax.shard_map(
        shards,
        mesh=mesh,
        in_specs=placed,
        out_specs=(
            P("pipe", "fsdp", "win", None, None),
            P("pipe", "fsdp", "win", None, None),
            P("pipe", None, ("win", "fsdp")),
            P("pipe", None, ("win", "fsdp")),
            P("pipe", ("win", "fsdp"), None),
            P("pipe", None, ("win", "fsdp")),
            P("pipe", None, None),
            P("pipe", ("win", "fsdp"), None),
            P("pipe", ("win", "fsdp"), None),
            P("pipe", ("win", "fsdp")),
            P("pipe", ("win", "fsdp"), None),
        ),
        check_vma=False,
    )
```
